32 devices in a mesh: section: 4 (over x, core), ep: 8 (over z, y).
Axes of the slice: x: 2, y: 2, z: 4, core: 2. Of those that a mesh axis runs over, the one named last changes fastest.
Arguments:
- output_grad: bfloat16 [4, 2048, 1024], P('section', 'ep'), may hold values from -6 to 6
- layer_input: bfloat16 [4, 2048, 1024], P('section', 'ep'), may hold values from -6 to 6
- expert_ids: int32 [4, 2048, 8], P('section', 'ep'), may hold values from 0 to 31, all different within a row; in each aligned block of 256 rows (0 to 255, 256 to 511, ..., all dimensions but the last counted through in order) at most 80 rows name the same one
- route_probs: bfloat16 [4, 2048, 8], P('section', 'ep'), may hold values from 0.049804688 to 0.44921875
- gate_weight: bfloat16 [4, 32, 1024, 384], P('section', 'ep'), may hold values from -0.1875 to 0.1875
- up_weight: bfloat16 [4, 32, 1024, 384], P('section', 'ep'), may hold values from -0.1875 to 0.1875
- down_weight: bfloat16 [4, 32, 384, 1024], P('section', 'ep'), may hold values from -0.3125 to 0.3125
- saved_inputs: bfloat16 [4, 32, 640, 1024], P('section', 'ep'), may hold values from -6 to 6
- saved_gate_grad: bfloat16 [4, 32, 640, 384], P('section', 'ep'), may hold values from -0.5 to 0.5
- saved_up_grad: bfloat16 [4, 32, 640, 384], P('section', 'ep'), may hold values from -0.5 to 0.5
- saved_counts: int32 [4, 32, 8], P('section', 'ep'), may hold values from 0 to 80, as said below
Outputs:
- upstream_grad: bfloat16 [4, 2048, 1024], P('section', 'ep')
- prob_grad: bfloat16 [4, 2048, 8], P('section', 'ep')
- gate_weight_grad: bfloat16 [4, 32, 1024, 384], P('section', 'ep')
- up_weight_grad: bfloat16 [4, 32, 1024, 384], P('section', 'ep')
The draws below stay inside these ranges and needn't reach their ends.
Inputs may be any that keep to these rules, and one draw needn't show every extreme that they name: `expert_ids`: each token names 8 different experts. Among the tokens of one device (aligned blocks of 256 tokens of a section) no expert is named more than 80 times, a bound that some block reaches. `saved_counts`: rows of a block at or beyond its count are padding; some block is full in every draw.
All inputs are finite; a program needn't handle non-finite values.
Results may differ from the reference program's by a relative error of at most 0.008.
Values may be sent and summed in bfloat16 or wider, within the bound.
A program may use at most 128 MiB of HBM per device.

```python
import math
import jax
import jax.numpy as jnp
import numpy as np
from jax import lax

D = 1024
FF = 384
TOP = 8
TOK_DEV = 256
SECTIONS = 4
TOKENS = 2048
EXPERTS = 32
SOURCES = 8
CAP = 80
SLOTS = 640
N_EP = 8


def draw_saved_counts(key, part):
    base = jax.random.randint(jax.random.fold_in(key, 11), (SECTIONS, EXPERTS, SOURCES), 0, CAP + 1)
    chosen = jax.random.randint(jax.random.fold_in(key, 12), (SECTIONS, 1, 1), 0, EXPERTS * SOURCES)
    flat = jnp.arange(EXPERTS * SOURCES, dtype=jnp.int32).reshape(1, EXPERTS, SOURCES)
    return jnp.where(flat == chosen, CAP, base).astype(jnp.int32)


def block_scale(rng, shape, shards, least, high):
    factor_of, own = 1.0, jax.random.fold_in(rng, 6)
    for axis_at, blocks in shards:
        draws = jnp.exp(jax.random.uniform(jax.random.fold_in(own, axis_at), (blocks,), jnp.float32, least / len(shards), high / len(shards)))
        factor_of = factor_of * jnp.repeat(draws, shape[axis_at] // blocks).reshape([-1 if axis == axis_at else 1 for axis in range(len(shape))])
    return factor_of


def deal_out(key, own, number, rows, amount, top, reach, slope):
    sequence = jax.random.permutation(key, amount)
    packed, common = shares(amount, rows * top, reach, slope, True), shares(amount, rows * top, reach, slope, False)
    places = jnp.arange(amount)

    def named(sizes, rotation):
        used = int((sizes > 0).sum())
        fixed = max(1, used // 4)
        passed = fixed + (places - fixed + rotation * (used - fixed)) % max(1, amount - fixed)
        return jnp.zeros((amount,), jnp.int32).at[sequence[jnp.where(places < fixed, places, passed)]].set(jnp.asarray(sizes, jnp.int32))

    sizes = jnp.where(number % 4 == 0, named(packed, number // 4), named(common, number - number // 4 - 1))
    mixed = jax.random.permutation(jax.random.fold_in(own, 3), amount)
    giver, receiver = mixed[0:amount // 2 * 2:2], mixed[1:amount // 2 * 2:2]
    slack = jnp.minimum(sizes[giver] - 1, reach - sizes[receiver]) // 2
    slack = jnp.where((giver == sequence[0]) | (receiver == sequence[0]) | (sizes[receiver] == 0), 0, jnp.maximum(slack, 0))
    passed = jax.random.randint(jax.random.fold_in(own, 4), (amount // 2,), 0, 1 << 20) % (slack + 1)
    sizes = sizes.at[giver].add(-passed).at[receiver].add(passed)
    labels = jnp.searchsorted(jnp.cumsum(sizes), jnp.arange(rows * top), side="right").astype(jnp.int32)
    grid = labels.reshape(top, rows).T
    grid = grid[jax.random.permutation(jax.random.fold_in(own, 1), rows)]
    rotation = jax.random.randint(jax.random.fold_in(own, 2), (rows, 1), 0, top)
    return jnp.take_along_axis(grid, (jnp.arange(top)[None, :] + rotation) % top, axis=1)


def shares(amount, total, limit, skew, full):
    weights = [(1 << 20) // math.isqrt(rank ** skew) + 1 for rank in range(1, amount + 1)]
    largest = limit if full else min(limit, max(-(-total // amount), total * weights[0] // sum(weights)))
    least = 1 if total - largest >= amount - 1 else 0
    given, spare = [largest] + [least] * (amount - 1), total - largest - least * (amount - 1)
    while spare > 0:
        free = [i for i in range(1, amount) if given[i] < largest] or [i for i in range(1, amount) if given[i] < limit]
        whole, budget = sum([weights[i] for i in free]), spare
        for i in free:
            more = min(limit - given[i], max(1, budget * weights[i] // whole), spare)
            given[i] = given[i] + more
            spare = spare - more
    return np.array(given)


def scatter_about(key, shape, deviation, reach, pieces=(), held_as=jnp.bfloat16):
    values = jax.random.normal(key, shape, jnp.float32) * deviation
    if len(pieces) > 0:
        values = block_scale(key, shape, pieces, -0.22, 0.18) * values
    return jnp.clip(values, min=-reach, max=reach).astype(held_as)


def setup_inputs(seed: int = 0) -> dict:
    splits = jax.random.split(jax.random.key(seed), 12)
    output_grad = scatter_about(splits[0], (SECTIONS, TOKENS, D), 1.0, 6.0, ((0, 4), (1, 8)))
    layer_input = scatter_about(splits[1], (SECTIONS, TOKENS, D), 1.0, 6.0, ((0, 4), (1, 8)))
    expert_ids_keys = jax.random.split(jax.random.fold_in(splits[2], 1), SECTIONS * TOKENS // TOK_DEV)
    expert_ids_turns = jax.random.permutation(jax.random.fold_in(splits[2], 3), SECTIONS * TOKENS // TOK_DEV)
    expert_ids = jax.vmap(lambda own, number: deal_out(jax.random.fold_in(splits[2], 2), own, number, TOK_DEV, EXPERTS, TOP, CAP, 2))(expert_ids_keys, expert_ids_turns).reshape((SECTIONS, TOKENS, TOP))
    route_probs = jnp.clip(0.049804688 + 0.39941406 * jax.random.uniform(splits[3], (SECTIONS, TOKENS, TOP), jnp.float32) ** block_scale(splits[3], (SECTIONS, TOKENS, TOP), ((0, 4), (1, 8)), -0.2, 0.2), 0.049804688, 0.44921875).astype(jnp.bfloat16)
    gate_weight = scatter_about(splits[4], (SECTIONS, EXPERTS, D, FF), D ** -0.5, 0.1875, ((0, 4), (1, 8)))
    up_weight = scatter_about(splits[5], (SECTIONS, EXPERTS, D, FF), D ** -0.5, 0.1875, ((0, 4), (1, 8)))
    down_weight = scatter_about(splits[6], (SECTIONS, EXPERTS, FF, D), FF ** -0.5, 0.3125, ((0, 4), (1, 8)))
    saved_inputs = scatter_about(splits[7], (SECTIONS, EXPERTS, SLOTS, D), 1.0, 6.0, ((0, 4), (1, 8)))
    saved_gate_grad = scatter_about(splits[8], (SECTIONS, EXPERTS, SLOTS, FF), 0.0625, 0.5, ((0, 4), (1, 8)))
    saved_up_grad = scatter_about(splits[9], (SECTIONS, EXPERTS, SLOTS, FF), 0.0625, 0.5, ((0, 4), (1, 8)))
    saved_counts = draw_saved_counts(jax.random.fold_in(splits[11], 71), 0)
    return {"output_grad": output_grad, "layer_input": layer_input, "expert_ids": expert_ids, "route_probs": route_probs, "gate_weight": gate_weight, "up_weight": up_weight, "down_weight": down_weight, "saved_inputs": saved_inputs, "saved_gate_grad": saved_gate_grad, "saved_up_grad": saved_up_grad, "saved_counts": saved_counts}


def block_slots(block_ids):
    flat_ids = block_ids.reshape(-1)
    onehot = (flat_ids[:, None] == jnp.arange(EXPERTS, dtype=jnp.int32)[None, :]).astype(jnp.int32)
    before = jnp.cumsum(onehot, axis=0) - onehot
    return jnp.sum(before * onehot, axis=1).astype(jnp.int32)


def expert_backward(operands):
    grad_rows, input_rows, prob_rows, w_gate, w_up, w_down = operands
    gate_pre = jnp.dot(input_rows, w_gate, preferred_element_type=jnp.float32)
    up_pre = jnp.dot(input_rows, w_up, preferred_element_type=jnp.float32)
    sigma = jax.nn.sigmoid(gate_pre)
    active = gate_pre * sigma
    hidden = (active * up_pre).astype(jnp.bfloat16)
    hidden_grad = jnp.dot(grad_rows, w_down.T, preferred_element_type=jnp.float32)
    output_rows = jnp.dot(hidden, w_down, preferred_element_type=jnp.float32)
    slot_prob = jnp.sum(output_rows * grad_rows.astype(jnp.float32), axis=1).astype(jnp.bfloat16)
    scaled = hidden_grad * prob_rows.astype(jnp.float32)[:, None]
    gate_grad = (scaled * up_pre * sigma * (1.0 + gate_pre * (1.0 - sigma))).astype(jnp.bfloat16)
    up_grad = (scaled * active).astype(jnp.bfloat16)
    slot_grad = jnp.dot(gate_grad, w_gate.T, preferred_element_type=jnp.float32)
    slot_grad = slot_grad + jnp.dot(up_grad, w_up.T, preferred_element_type=jnp.float32)
    return slot_grad.astype(jnp.bfloat16), slot_prob


def weight_pair(operands):
    masked, gate_grad, up_grad = operands
    gate_part = jnp.dot(masked.T, gate_grad, preferred_element_type=jnp.float32).astype(jnp.bfloat16)
    up_part = jnp.dot(masked.T, up_grad, preferred_element_type=jnp.float32).astype(jnp.bfloat16)
    return gate_part, up_part


def section_pass(grad, inputs, ids, probs, w_gate, w_up, w_down):
    blocks = ids.reshape(N_EP, TOK_DEV * TOP)
    slots = jax.vmap(block_slots)(blocks)
    source = jnp.arange(N_EP, dtype=jnp.int32)[:, None]
    place = (blocks * SLOTS + source * CAP + slots).reshape(-1).astype(jnp.int32)
    token = (jnp.arange(TOKENS * TOP, dtype=jnp.int32) // TOP).astype(jnp.int32)
    grad_rows = jnp.zeros((EXPERTS * SLOTS, D), jnp.bfloat16).at[place].set(grad[token])
    input_rows = jnp.zeros((EXPERTS * SLOTS, D), jnp.bfloat16).at[place].set(inputs[token])
    prob_rows = jnp.zeros((EXPERTS * SLOTS,), jnp.bfloat16).at[place].set(probs.reshape(-1))
    slot_grad, slot_prob = lax.map(expert_backward, (grad_rows.reshape(EXPERTS, SLOTS, D), input_rows.reshape(EXPERTS, SLOTS, D), prob_rows.reshape(EXPERTS, SLOTS), w_gate, w_up, w_down))
    picked = slot_grad.reshape(EXPERTS * SLOTS, D)[place]
    input_grad = jnp.sum(picked.reshape(TOKENS, TOP, D).astype(jnp.float32), axis=1).astype(jnp.bfloat16)
    prob_part = slot_prob.reshape(-1)[place].reshape(TOKENS, TOP)
    return input_grad, prob_part


def weight_pass(inputs, gate_grad, up_grad, counts):
    capacity = jnp.arange(CAP, dtype=jnp.int32)
    live = (capacity[None, None, :] < counts[:, :, None]).reshape(EXPERTS, SLOTS)
    masked = inputs * live.astype(jnp.bfloat16)[:, :, None]
    return lax.map(weight_pair, (masked, gate_grad, up_grad))


def reference(output_grad, layer_input, expert_ids, route_probs, gate_weight, up_weight, down_weight, saved_inputs, saved_gate_grad, saved_up_grad, saved_counts):
    input_grads = []
    prob_grads = []
    gate_grads = []
    up_grads = []
    for section_index in range(SECTIONS):
        input_grad, prob_part = section_pass(output_grad[section_index], layer_input[section_index], expert_ids[section_index], route_probs[section_index], gate_weight[section_index], up_weight[section_index], down_weight[section_index])
        gate_part, up_part = weight_pass(saved_inputs[section_index], saved_gate_grad[section_index], saved_up_grad[section_index], saved_counts[section_index])
        input_grads.append(input_grad)
        prob_grads.append(prob_part)
        gate_grads.append(gate_part)
        up_grads.append(up_part)
    stacked = jnp.stack(input_grads)
    upstream_grad = jnp.concatenate([stacked[1:], jnp.zeros_like(stacked[:1])], axis=0)
    return upstream_grad, jnp.stack(prob_grads), jnp.stack(gate_grads), jnp.stack(up_grads)
```

```python
import jax
import jax.numpy as jnp
from jax import lax
from jax.sharding import PartitionSpec as P

F32 = jnp.float32
BF16 = jnp.bfloat16


def from_behind(array, axis, by):
    devices = lax.axis_size(axis)
    pairs = [(i, i + by) for i in range(devices) if 0 <= i + by < devices]
    return lax.ppermute(array, axis, pairs)


def per_device(
    output_grad,
    layer_input,
    expert_ids,
    route_probs,
    gate_weight,
    up_weight,
    down_weight,
    saved_inputs,
    saved_gate_grad,
    saved_up_grad,
    saved_counts,
):
    ep_count = lax.axis_size("ep")
    me = lax.axis_index("ep")
    w_gate = gate_weight[0]
    w_up = up_weight[0]
    w_down = down_weight[0]
    local_experts = w_gate.shape[0]
    experts_all = local_experts * ep_count
    slots_all = saved_inputs.shape[2]
    capacity = slots_all // ep_count
    tok_rows = expert_ids.shape[1]
    top_count = expert_ids.shape[2]
    width = output_grad.shape[2]

    small = jnp.concatenate([expert_ids[0].astype(BF16), route_probs[0]], axis=1)
    small = jnp.pad(small, ((0, 0), (0, 128 - small.shape[1])))
    packed = jnp.concatenate([output_grad[0], layer_input[0], small], axis=1)
    everyone = lax.all_gather(packed, "ep", axis=0, tiled=False)

    live = jnp.arange(capacity, dtype=jnp.int32)[None, None, :] < saved_counts[0][:, :, None]
    masked = saved_inputs[0] * live.reshape(local_experts, slots_all).astype(BF16)[:, :, None]
    gate_part = jnp.einsum(
        "esd,esf->edf", masked, saved_gate_grad[0], preferred_element_type=F32
    ).astype(BF16)
    up_part = jnp.einsum(
        "esd,esf->edf", masked, saved_up_grad[0], preferred_element_type=F32
    ).astype(BF16)

    ids_all = everyone[:, :, 2 * width : 2 * width + top_count].astype(jnp.int32)
    probs_all = everyone[:, :, 2 * width + top_count : 2 * width + 2 * top_count].astype(F32)
    mine = me * local_experts + jnp.arange(local_experts, dtype=jnp.int32)
    hit = ids_all[:, None, :, :] == mine[None, :, None, None]
    member = jnp.any(hit, axis=3)
    prob = jnp.sum(jnp.where(hit, probs_all[:, None], 0.0), axis=3)
    lower = jnp.tril(jnp.ones((tok_rows, tok_rows), BF16), -1)
    before = jnp.einsum("sen,tn->set", member.astype(BF16), lower, preferred_element_type=F32)
    slot = jnp.where(member, before.astype(jnp.int32), -1)
    chosen = slot[:, :, None, :] == jnp.arange(capacity, dtype=jnp.int32)[None, None, :, None]
    pick = chosen.astype(BF16)
    put = jnp.where(chosen, prob[:, :, None, :], 0.0).astype(BF16)
    rows = jnp.einsum(
        "sect,std->escd", pick, everyone[:, :, : 2 * width], preferred_element_type=F32
    ).astype(BF16)
    rows = rows.reshape(local_experts, slots_all, 2 * width)
    grad_part = rows[:, :, :width]
    input_part = rows[:, :, width:]

    gate_pre = jnp.einsum("epd,edf->epf", input_part, w_gate, preferred_element_type=F32)
    up_pre = jnp.einsum("epd,edf->epf", input_part, w_up, preferred_element_type=F32)
    sigma = jax.nn.sigmoid(gate_pre)
    active = gate_pre * sigma
    hidden = active * up_pre
    hidden_grad = jnp.einsum("epd,efd->epf", grad_part, w_down, preferred_element_type=F32)
    slot_prob = jnp.sum(hidden_grad * hidden, axis=2).astype(BF16)
    gate_grad = (hidden_grad * up_pre * sigma * (1.0 + gate_pre * (1.0 - sigma))).astype(BF16)
    up_grad = (hidden_grad * active).astype(BF16)
    slot_grad = jnp.einsum("epf,edf->epd", gate_grad, w_gate, preferred_element_type=F32)
    slot_grad = slot_grad + jnp.einsum("epf,edf->epd", up_grad, w_up, preferred_element_type=F32)
    slot_grad = slot_grad.astype(BF16).reshape(local_experts, ep_count, capacity, width)
    token_grad = jnp.einsum("sect,escd->std", put, slot_grad, preferred_element_type=F32)
    slot_prob = slot_prob.reshape(local_experts, ep_count, capacity)
    token_prob = jnp.einsum("sect,esc->ste", pick, slot_prob, preferred_element_type=F32)
    spread = jnp.where(
        (jnp.arange(ep_count) == me)[None, None, :, None], token_prob[:, :, None, :], 0.0
    ).reshape(ep_count, tok_rows, experts_all)
    pad = -experts_all % 128
    back = jnp.concatenate([token_grad, jnp.pad(spread, ((0, 0), (0, 0), (0, pad)))], axis=2)
    summed = lax.psum_scatter(back.astype(BF16), "ep", scatter_dimension=0, tiled=False)
    input_grad = summed[:, :width]
    own = expert_ids[0][:, :, None] == jnp.arange(experts_all, dtype=jnp.int32)[None, None, :]
    prob_part = jnp.sum(
        jnp.where(own, summed[:, None, width : width + experts_all].astype(F32), 0.0), axis=2
    ).astype(BF16)
    upstream = from_behind(input_grad[None], "section", -1)
    return (upstream, prob_part[None], gate_part[None], up_part[None])


def solution(mesh):
    three = P("section", "ep", None)
    four = P("section", "ep", None, None)
    return jax.shard_map(
        per_device,
        mesh=mesh,
        in_specs=(three, three, three, three, four, four, four, four, four, four, three),
        out_specs=(three, three, four, four),
        check_vma=False,
    )
```

```python
import functools

import jax
import jax.numpy as jnp
from jax import lax
from jax.experimental import pallas as pl
from jax.experimental.pallas import tpu as pltpu
from jax.sharding import PartitionSpec as P

F32 = jnp.float32
BF16 = jnp.bfloat16
MESH = pl.DeviceIdType.MESH
VMEM = pl.BlockSpec(memory_space=pltpu.VMEM)
ANY = pl.BlockSpec(memory_space=pl.ANY)


class Copies:
    def __init__(self, send, recv):
        self.send, self.recv, self.used, self.items = send, recv, 0, []

    def make(self, src, dst, target):
        at = self.used
        self.used += 1
        copy = pltpu.make_async_remote_copy(
            src_ref=src,
            dst_ref=dst,
            send_sem=self.send.at[at],
            recv_sem=self.recv.at[at],
            device_id=target,
            device_id_type=MESH,
        )
        self.items.append(copy)
        return copy

    def start(self, src, dst, target):
        copy = self.make(src, dst, target)
        copy.start()
        return copy


def place_of(count):
    me = lax.axis_index("ep")
    outer, inner = me // 2, me % 2
    ring = count // 2
    up = ((outer + 1) % ring) * 2 + inner
    down = ((outer + ring - 1) % ring) * 2 + inner
    return me, outer, inner, ring, (up, down), outer * 2 + 1 - inner


def gather_copies(count):
    ring = count // 2
    return 6 * (ring - 1) + 2 * (ring - 1) + 2 + (count - 1)


def gather_kernel(count, g, x, s, g_all, x_all, s_all, local, send, recv):
    me, outer, inner, ring, sides, partner = place_of(count)
    tokens = g.shape[0]
    half = tokens // 2
    rows = (pl.ds(0, half), pl.ds(half, half))
    copies = Copies(send, recv)
    own = [
        pltpu.make_async_copy(g, g_all.at[me], local.at[0]),
        pltpu.make_async_copy(x, x_all.at[me], local.at[1]),
        pltpu.make_async_copy(s, s_all.at[me], local.at[2]),
    ]
    for copy in own:
        copy.start()
    barrier = pltpu.get_barrier_semaphore()
    for away in range(1, count):
        pl.semaphore_signal(
            barrier, inc=1, device_id={"ep": (me + away) % count}, device_id_type=MESH
        )
    pl.semaphore_wait(barrier, count - 1)

    def block(step, side, row):
        return ((outer + (-step if side == 0 else step) + ring) % ring) * 2 + row

    def hop(ref, all_ref, step, side, row):
        at = block(step, side, row)
        dst = all_ref.at[at, rows[side]]
        source = dst if ref is None else ref.at[rows[side]]
        return copies.start(source, dst, {"ep": sides[side]})

    side_list = (0, 1)
    other = 1 - inner
    x_now = [hop(x, x_all, 0, side, inner) for side in side_list]
    g_across = copies.start(g, g_all.at[me], {"ep": partner})
    g_now = [hop(g, g_all, 0, side, inner) for side in side_list]
    x_across = copies.start(x, x_all.at[me], {"ep": partner})
    tiny = [
        copies.start(s, s_all.at[me], {"ep": (me + away) % count}) for away in range(1, count)
    ]
    g_other = None
    late = [x_across] + tiny
    for step in range(ring - 1):
        more = step < ring - 2
        x_next = []
        for side in side_list:
            x_now[side].wait_recv()
            if more:
                x_next.append(hop(None, x_all, step + 1, side, inner))
            got = x_all.at[block(step + 1, side, inner), rows[side]]
            late.append(copies.start(got, got, {"ep": partner}))
        x_now = x_next
        g_next = []
        for side in side_list:
            g_now[side].wait_recv()
            if more:
                g_next.append(hop(None, g_all, step + 1, side, inner))
        g_now = g_next
        if step == 0:
            g_across.wait_recv()
        else:
            for copy in g_other:
                copy.wait_recv()
        g_other = [hop(None, g_all, step, side, other) for side in side_list]
    for copy in g_other + late:
        copy.wait_recv()
    for copy in copies.items:
        copy.wait_send()
    for copy in own:
        copy.wait()


def gather_tokens(count, g, x, s):
    pairs = gather_copies(count)
    return pl.pallas_call(
        functools.partial(gather_kernel, count),
        out_shape=[jax.ShapeDtypeStruct((count,) + a.shape, a.dtype) for a in (g, x, s)],
        in_specs=[VMEM] * 3,
        out_specs=[ANY] * 3,
        scratch_shapes=[
            pltpu.SemaphoreType.DMA((3,)),
            pltpu.SemaphoreType.DMA((pairs,)),
            pltpu.SemaphoreType.DMA((pairs,)),
        ],
        compiler_params=pltpu.CompilerParams(collective_id=0, has_side_effects=True),
    )(g, x, s)


def scatter_copies(count):
    ring = count // 2
    return 6 * (ring - 1) + ring + 2 + (count - 1)


def add(a, b):
    return (a.astype(F32) + b.astype(F32)).astype(BF16)


def scatter_kernel(
    count, sections, part, prob, out, prob_out, a_ring, b_ring, b_across, a_take, land,
    total, send, recv, shift_send, shift_recv,
):
    me, outer, inner, ring, sides, partner = place_of(count)
    section = lax.axis_index("section")
    tokens, width = out.shape
    half, wide = tokens // 2, width // 2
    rows = (pl.ds(0, half), pl.ds(half, half))
    left, right = pl.ds(0, wide), pl.ds(wide, wide)
    copies = Copies(send, recv)
    barrier = pltpu.get_barrier_semaphore()
    for away in range(1, count):
        pl.semaphore_signal(
            barrier, inc=1, device_id={"ep": (me + away) % count}, device_id_type=MESH
        )
    for away in (1, sections - 1):
        pl.semaphore_signal(
            barrier, inc=1, device_id={"section": (section + away) % sections}, device_id_type=MESH
        )
    pl.semaphore_wait(barrier, count + 1)
    other = 1 - inner
    side_list = (0, 1)

    def goal(step, side):
        return (outer + (-1 - step if side == 0 else 1 + step) + 2 * ring) % ring

    a_now = {}
    for row, which in ((other, 0), (inner, 1)):
        for side in side_list:
            a_now[which, side] = copies.start(
                part.at[goal(0, side) * 2 + row, rows[side], left],
                a_ring.at[which, side, 0],
                {"ep": sides[side]},
            )
    across = {}
    order = []
    for step in range(ring - 1):
        for side in side_list:
            at = (-1 - step if side == 0 else 1 + step) % ring
            if at not in order:
                order.append(at)
    order.append(0)
    for at in order:
        place = (outer + at) % ring
        across[at] = copies.start(
            part.at[place * 2 + other, :, right], b_across.at[at], {"ep": partner}
        )
    tiny = [
        copies.start(
            prob.at[(me + away) % count], prob_out.at[me], {"ep": (me + away) % count}
        )
        for away in range(1, count)
    ]
    prob_out[me] = prob[me]
    summed = []

    def settle(at):
        if at not in summed:
            summed.append(at)
            across[at].wait_recv()
            place = (outer + at) % ring
            b_across[at] = add(b_across[at], part[place * 2 + inner, :, wide:])

    b_now = {}
    for side in side_list:
        at = (-1 if side == 0 else 1) % ring
        settle(at)
        b_now[side] = copies.start(
            b_across.at[at, rows[side]], b_ring.at[side, 0], {"ep": sides[side]}
        )
    for step in range(ring - 1):
        more = step < ring - 2
        for which, row in ((0, other), (1, inner)):
            for side in side_list:
                place = goal(step + 1, side)
                span = slice(side * half, (side + 1) * half)
                a_now[which, side].wait_recv()
                a_ring[which, side, step] = add(
                    a_ring[which, side, step], part[place * 2 + row, span, :wide]
                )
                if more:
                    a_now[which, side] = copies.start(
                        a_ring.at[which, side, step],
                        a_ring.at[which, side, step + 1],
                        {"ep": sides[side]},
                    )
                elif which == 0:
                    a_now[which, side] = copies.start(
                        a_ring.at[which, side, step], a_take.at[rows[side]], {"ep": partner}
                    )
        for side in side_list:
            at = (-2 - step if side == 0 else 2 + step) % ring
            settle(at)
            span = slice(side * half, (side + 1) * half)
            b_now[side].wait_recv()
            if more:
                b_ring[side, step] = add(b_ring[side, step], b_across[at, span])
                b_now[side] = copies.start(
                    b_ring.at[side, step], b_ring.at[side, step + 1], {"ep": sides[side]}
                )
            else:
                total[1, span] = add(b_ring[side, step], b_across[at, span])

    def shift(column):
        return pltpu.make_async_remote_copy(
            src_ref=total.at[column],
            dst_ref=land.at[column],
            send_sem=shift_send.at[column],
            recv_sem=shift_recv.at[column],
            device_id={"section": (section + sections - 1) % sections},
            device_id_type=MESH,
        )

    @pl.when(section > 0)
    def _():
        shift(1).start()

    for side in side_list:
        span = slice(side * half, (side + 1) * half)
        a_now[0, side].wait_recv()
        total[0, span] = add(a_ring[1, side, ring - 2], a_take[span])

    @pl.when(section > 0)
    def _():
        shift(0).start()

    for copy in tiny:
        copy.wait_recv()
    for copy in copies.items:
        copy.wait_send()

    @pl.when(section > 0)
    def _():
        shift(1).wait_send()
        shift(0).wait_send()

    @pl.when(section < sections - 1)
    def _():
        shift(1).wait_recv()
        out[:, wide:] = land[1]
        shift(0).wait_recv()
        out[:, :wide] = land[0]

    @pl.when(section == sections - 1)
    def _():
        out[...] = jnp.zeros_like(out)


def scatter_tokens(count, sections, part, prob):
    pairs = scatter_copies(count)
    ring = count // 2
    _, tokens, width = part.shape
    half, wide = tokens // 2, width // 2
    return pl.pallas_call(
        functools.partial(scatter_kernel, count, sections),
        out_shape=[
            jax.ShapeDtypeStruct((tokens, width), BF16),
            jax.ShapeDtypeStruct(prob.shape, prob.dtype),
        ],
        in_specs=[VMEM] * 2,
        out_specs=[VMEM] * 2,
        scratch_shapes=[
            pltpu.VMEM((2, 2, ring - 1, half, wide), BF16),
            pltpu.VMEM((2, ring - 1, half, wide), BF16),
            pltpu.VMEM((ring, tokens, wide), BF16),
            pltpu.VMEM((tokens, wide), BF16),
            pltpu.VMEM((2, tokens, wide), BF16),
            pltpu.VMEM((2, tokens, wide), BF16),
            pltpu.SemaphoreType.DMA((pairs,)),
            pltpu.SemaphoreType.DMA((pairs,)),
            pltpu.SemaphoreType.DMA((2,)),
            pltpu.SemaphoreType.DMA((2,)),
        ],
        compiler_params=pltpu.CompilerParams(
            collective_id=1, has_side_effects=True, vmem_limit_bytes=40 * 1024 * 1024
        ),
    )(part, prob)


def per_device(
    output_grad,
    layer_input,
    expert_ids,
    route_probs,
    gate_weight,
    up_weight,
    down_weight,
    saved_inputs,
    saved_gate_grad,
    saved_up_grad,
    saved_counts,
):
    ep_count = lax.axis_size("ep")
    sections = lax.axis_size("section")
    me = lax.axis_index("ep")
    w_gate = gate_weight[0]
    w_up = up_weight[0]
    w_down = down_weight[0]
    local_experts = w_gate.shape[0]
    experts_all = local_experts * ep_count
    slots_all = saved_inputs.shape[2]
    capacity = slots_all // ep_count
    tok_rows = expert_ids.shape[1]
    top_count = expert_ids.shape[2]
    width = output_grad.shape[2]

    small = jnp.concatenate([expert_ids[0].astype(BF16), route_probs[0]], axis=1).T
    grad_all, input_all, small_all = gather_tokens(
        ep_count, output_grad[0], layer_input[0], small
    )

    live = jnp.arange(capacity, dtype=jnp.int32)[None, None, :] < saved_counts[0][:, :, None]
    masked = saved_inputs[0] * live.reshape(local_experts, slots_all).astype(BF16)[:, :, None]
    gate_part = jnp.einsum(
        "esd,esf->edf", masked, saved_gate_grad[0], preferred_element_type=F32
    ).astype(BF16)
    up_part = jnp.einsum(
        "esd,esf->edf", masked, saved_up_grad[0], preferred_element_type=F32
    ).astype(BF16)

    ids_all = small_all[:, :top_count].astype(jnp.int32)
    probs_all = small_all[:, top_count:].astype(F32)
    mine = me * local_experts + jnp.arange(local_experts, dtype=jnp.int32)
    hit = ids_all[:, None, :, :] == mine[None, :, None, None]
    member = jnp.any(hit, axis=2)
    prob = jnp.sum(jnp.where(hit, probs_all[:, None], 0.0), axis=2)
    lower = jnp.tril(jnp.ones((tok_rows, tok_rows), BF16), -1)
    before = jnp.einsum("sen,tn->set", member.astype(BF16), lower, preferred_element_type=F32)
    slot = jnp.where(member, before.astype(jnp.int32), -1)
    chosen = slot[:, :, None, :] == jnp.arange(capacity, dtype=jnp.int32)[None, None, :, None]
    pick = chosen.astype(BF16).reshape(ep_count, local_experts * capacity, tok_rows)
    put = jnp.where(chosen, prob[:, :, None, :], 0.0).astype(BF16)
    put = put.reshape(ep_count, local_experts * capacity, tok_rows)

    def spread(tokens):
        sent = jnp.einsum("spt,std->spd", pick, tokens, preferred_element_type=F32).astype(BF16)
        sent = sent.reshape(ep_count, local_experts, capacity, width)
        return sent.transpose(1, 0, 2, 3).reshape(local_experts, slots_all, width)

    grad_part = spread(grad_all)
    input_part = spread(input_all)

    gate_pre = jnp.einsum("epd,edf->epf", input_part, w_gate, preferred_element_type=F32)
    up_pre = jnp.einsum("epd,edf->epf", input_part, w_up, preferred_element_type=F32)
    sigma = jax.nn.sigmoid(gate_pre)
    active = gate_pre * sigma
    hidden = active * up_pre
    hidden_grad = jnp.einsum("epd,efd->epf", grad_part, w_down, preferred_element_type=F32)
    slot_prob = jnp.sum(hidden_grad * hidden, axis=2).astype(BF16)
    gate_grad = (hidden_grad * up_pre * sigma * (1.0 + gate_pre * (1.0 - sigma))).astype(BF16)
    up_grad = (hidden_grad * active).astype(BF16)
    slot_grad = jnp.einsum("epf,edf->epd", gate_grad, w_gate, preferred_element_type=F32)
    slot_grad = slot_grad + jnp.einsum("epf,edf->epd", up_grad, w_up, preferred_element_type=F32)
    slot_grad = slot_grad.astype(BF16).reshape(local_experts, ep_count, capacity, width)
    slot_grad = slot_grad.transpose(1, 0, 2, 3).reshape(ep_count, -1, width)
    token_grad = jnp.einsum("spt,spd->std", put, slot_grad, preferred_element_type=F32)
    slot_prob = slot_prob.reshape(local_experts, ep_count, capacity)
    by_slot = chosen.astype(BF16)
    token_prob = jnp.einsum("sect,esc->set", by_slot, slot_prob, preferred_element_type=F32)
    upstream, prob_back = scatter_tokens(
        ep_count, sections, token_grad.astype(BF16), token_prob.astype(BF16)
    )
    prob_back = prob_back.reshape(experts_all, tok_rows)
    own = expert_ids[0][None, :, :] == jnp.arange(experts_all, dtype=jnp.int32)[:, None, None]
    prob_part = jnp.sum(jnp.where(own, prob_back[:, :, None].astype(F32), 0.0), axis=0)
    prob_part = prob_part.astype(BF16)
    upstream = upstream[None]
    return (upstream, prob_part[None], gate_part[None], up_part[None])


def solution(mesh):
    three = P("section", "ep", None)
    four = P("section", "ep", None, None)
    return jax.shard_map(
        per_device,
        mesh=mesh,
        in_specs=(three, three, three, three, four, four, four, four, four, four, three),
        out_specs=(three, three, four, four),
        check_vma=False,
    )
```

```python
import functools

import jax
import jax.numpy as jnp
from jax import lax
from jax.experimental import pallas as pl
from jax.experimental.pallas import tpu as pltpu
from jax.sharding import PartitionSpec as P

F32 = jnp.float32
BF16 = jnp.bfloat16
MESH = pl.DeviceIdType.MESH
VMEM = pl.BlockSpec(memory_space=pltpu.VMEM)
ANY = pl.BlockSpec(memory_space=pl.ANY)


class Copies:
    def __init__(self, send, recv):
        self.send, self.recv, self.used, self.items = send, recv, 0, []

    def start(self, src, dst, target, when=None):
        at = self.used
        self.used += 1
        copy = pltpu.make_async_remote_copy(
            src_ref=src,
            dst_ref=dst,
            send_sem=self.send.at[at],
            recv_sem=self.recv.at[at],
            device_id={"ep": target},
            device_id_type=MESH,
        )
        self.items.append((copy, when))
        guarded(when, copy.start)
        return copy

    def finish(self):
        for copy, when in self.items:
            guarded(when, copy.wait_send)


def guarded(when, act):
    if when is None:
        act()
    else:
        pl.when(when)(act)


def place_of(count):
    me = lax.axis_index("ep")
    outer, inner = me // 2, me % 2
    line = count // 2
    up = ((outer + 1) % line) * 2 + inner
    down = ((outer + line - 1) % line) * 2 + inner
    return me, outer, inner, line, (up, down), outer * 2 + 1 - inner


def gather_copies(count):
    line = count // 2
    return 12 * (line - 1) + 3 + (count - 1)


def gather_kernel(count, g, x, s, g_all, x_all, s_all, local, send, recv):
    me, outer, inner, line, sides, partner = place_of(count)
    width = g.shape[1]
    cut = max(width * 3 // 1024, 1) * 128
    copies = Copies(send, recv)
    own = [
        pltpu.make_async_copy(g, g_all.at[me], local.at[0]),
        pltpu.make_async_copy(x, x_all.at[me], local.at[1]),
        pltpu.make_async_copy(s, s_all.at[me], local.at[2]),
    ]
    for copy in own:
        copy.start()
    barrier = pltpu.get_barrier_semaphore()
    for away in range(1, count):
        pl.semaphore_signal(
            barrier, inc=1, device_id={"ep": (me + away) % count}, device_id_type=MESH
        )
    pl.semaphore_wait(barrier, count - 1)
    everything, few, many = pl.ds(0, width), pl.ds(0, cut), pl.ds(cut, width - cut)

    def block(step, side):
        return (outer + (-step if side == 0 else step) + 2 * line) % line

    def arrives(step, side):
        return outer >= step + 1 if side == 0 else outer + step + 1 <= line - 1

    def leaves(step, side):
        if side == 0:
            return jnp.logical_and(outer >= step, outer < line - 1)
        return jnp.logical_and(outer + step <= line - 1, outer > 0)

    def hop(ref, all_ref, columns, step, side, row):
        dst = all_ref.at[block(step, side) * 2 + row, :, columns]
        source = dst if ref is None else ref.at[:, columns]
        return copies.start(source, dst, sides[side], leaves(step, side))

    def take(copy, step, side):
        guarded(arrives(step, side), copy.wait_recv)

    side_list = (0, 1)
    other = 1 - inner
    pieces = ((x, x_all, everything), (g, g_all, many))
    now = {}
    g_across = copies.start(g.at[:, few], g_all.at[me, :, few], partner)
    for at, (ref, all_ref, columns) in enumerate(pieces):
        for side in side_list:
            now[at, side] = hop(ref, all_ref, columns, 0, side, inner)
    for side in side_list:
        now[2, side] = hop(g, g_all, few, 0, side, inner)
    late = [
        (copies.start(x, x_all.at[me], partner), None),
        (copies.start(g.at[:, many], g_all.at[me, :, many], partner), None),
    ]
    for away in range(1, count):
        late.append((copies.start(s, s_all.at[me], (me + away) % count), None))
    g_across.wait_recv()
    for side in side_list:
        now[3, side] = hop(None, g_all, few, 0, side, other)
    for step in range(line - 1):
        more = step < line - 2
        for at in range(4):
            row = other if at == 3 else inner
            all_ref, columns = pieces[at][1:] if at < 2 else (g_all, few)
            for side in side_list:
                take(now[at, side], step, side)
                if more:
                    now[at, side] = hop(None, all_ref, columns, step + 1, side, row)
                if at < 2:
                    got = all_ref.at[block(step + 1, side) * 2 + inner, :, columns]
                    has = arrives(step, side)
                    late.append((copies.start(got, got, partner, has), has))
    for copy, when in late:
        guarded(when, copy.wait_recv)
    copies.finish()
    for copy in own:
        copy.wait()


def gather_tokens(count, g, x, s):
    pairs = gather_copies(count)
    return pl.pallas_call(
        functools.partial(gather_kernel, count),
        out_shape=[jax.ShapeDtypeStruct((count,) + a.shape, a.dtype) for a in (g, x, s)],
        in_specs=[VMEM] * 3,
        out_specs=[ANY] * 3,
        scratch_shapes=[
            pltpu.SemaphoreType.DMA((3,)),
            pltpu.SemaphoreType.DMA((pairs,)),
            pltpu.SemaphoreType.DMA((pairs,)),
        ],
        compiler_params=pltpu.CompilerParams(collective_id=0, has_side_effects=True),
    )(g, x, s)


def scatter_copies(count):
    line = count // 2
    return line + 1 + (count - 1)


def add(a, b):
    return (a.astype(F32) + b.astype(F32)).astype(BF16)


def scatter_kernel(
    count, sections, part, prob, out, prob_out, a_sum, a_side, a_take, b_sum, b_side, land_a,
    land_b, send, recv, line_send, line_recv, shift_send, shift_recv,
):
    me, outer, inner, line, sides, partner = place_of(count)
    section = lax.axis_index("section")
    cut = a_sum.shape[3]
    copies = Copies(send, recv)
    barrier = pltpu.get_barrier_semaphore()
    for away in range(1, count):
        pl.semaphore_signal(
            barrier, inc=1, device_id={"ep": (me + away) % count}, device_id_type=MESH
        )
    for away in (1, sections - 1):
        pl.semaphore_signal(
            barrier, inc=1, device_id={"section": (section + away) % sections}, device_id_type=MESH
        )
    pl.semaphore_wait(barrier, count + 1)
    other = 1 - inner
    low, high = pl.ds(0, cut), pl.ds(cut, part.shape[2] - cut)

    def goal(at):
        mixed = line - 1 - at // 2 if at % 2 == 0 else at // 2
        return jnp.where(outer == 0, line - 1 - at, jnp.where(outer == line - 1, at, mixed))

    across = [
        copies.start(part.at[goal(at) * 2 + other, :, high], b_sum.at[goal(at)], partner)
        for at in range(line)
    ]
    tiny = [
        copies.start(prob.at[(me + away) % count], prob_out.at[me], (me + away) % count)
        for away in range(1, count)
    ]
    prob_out[me] = prob[me]

    def line_copy(kind, source, side_ref, side, place):
        return pltpu.make_async_remote_copy(
            src_ref=source.at[place],
            dst_ref=side_ref.at[side, place],
            send_sem=line_send.at[kind, side, place],
            recv_sem=line_recv.at[kind, side, place],
            device_id={"ep": sides[side]},
            device_id_type=MESH,
        )

    def collect(kind, total, side_ref, side, place):
        line_copy(kind, total, side_ref, side, place).wait_recv()
        total[place] = add(total[place], side_ref[side, place])

    def advance(kind, total, side_ref, place):
        @pl.when(jnp.logical_and(place >= outer, outer > 0))
        def _():
            collect(kind, total, side_ref, 0, place)

        @pl.when(jnp.logical_and(place <= outer, outer < line - 1))
        def _():
            collect(kind, total, side_ref, 1, place)

        @pl.when(place > outer)
        def _():
            line_copy(kind, total, side_ref, 0, place).start()

        @pl.when(place < outer)
        def _():
            line_copy(kind, total, side_ref, 1, place).start()

    for at in range(line):
        place = goal(at)
        for kind, row in ((0, other), (1, inner)):
            a_sum[kind, place] = part[place * 2 + row, :, :cut]
            advance(kind, a_sum.at[kind], a_side.at[kind], place)
    a_across = copies.start(a_sum.at[0, outer], a_take, partner)
    for at in range(line):
        place = goal(at)
        across[at].wait_recv()
        b_sum[place] = add(b_sum[place], part[place * 2 + inner, :, cut:])
        advance(2, b_sum, b_side, place)

    def shift(column, source, land):
        return pltpu.make_async_remote_copy(
            src_ref=source,
            dst_ref=land,
            send_sem=shift_send.at[column],
            recv_sem=shift_recv.at[column],
            device_id={"section": (section + sections - 1) % sections},
            device_id_type=MESH,
        )

    a_across.wait_recv()
    a_sum[1, outer] = add(a_sum[1, outer], a_take[...])
    shifts = (shift(0, a_sum.at[1, outer], land_a), shift(1, b_sum.at[outer], land_b))

    @pl.when(section > 0)
    def _():
        for copy in shifts:
            copy.start()

    for copy in tiny:
        copy.wait_recv()
    copies.finish()
    for place in range(line):
        for kind, total, side_ref in (
            (0, a_sum.at[0], a_side.at[0]),
            (1, a_sum.at[1], a_side.at[1]),
            (2, b_sum, b_side),
        ):
            guarded(place > outer, line_copy(kind, total, side_ref, 0, place).wait_send)
            guarded(place < outer, line_copy(kind, total, side_ref, 1, place).wait_send)

    @pl.when(section > 0)
    def _():
        for copy in shifts:
            copy.wait_send()

    @pl.when(section < sections - 1)
    def _():
        shifts[0].wait_recv()
        out[:, :cut] = land_a[...]
        shifts[1].wait_recv()
        out[:, cut:] = land_b[...]

    @pl.when(section == sections - 1)
    def _():
        out[...] = jnp.zeros_like(out)


def scatter_tokens(count, sections, part, prob):
    pairs = scatter_copies(count)
    line = count // 2
    _, tokens, width = part.shape
    cut = max(width // 1024, 1) * 128
    rest = width - cut
    return pl.pallas_call(
        functools.partial(scatter_kernel, count, sections),
        out_shape=[
            jax.ShapeDtypeStruct((tokens, width), BF16),
            jax.ShapeDtypeStruct(prob.shape, prob.dtype),
        ],
        in_specs=[VMEM] * 2,
        out_specs=[VMEM] * 2,
        scratch_shapes=[
            pltpu.VMEM((2, line, tokens, cut), BF16),
            pltpu.VMEM((2, 2, line, tokens, cut), BF16),
            pltpu.VMEM((tokens, cut), BF16),
            pltpu.VMEM((line, tokens, rest), BF16),
            pltpu.VMEM((2, line, tokens, rest), BF16),
            pltpu.VMEM((tokens, cut), BF16),
            pltpu.VMEM((tokens, rest), BF16),
            pltpu.SemaphoreType.DMA((pairs,)),
            pltpu.SemaphoreType.DMA((pairs,)),
            pltpu.SemaphoreType.DMA((3, 2, line)),
            pltpu.SemaphoreType.DMA((3, 2, line)),
            pltpu.SemaphoreType.DMA((2,)),
            pltpu.SemaphoreType.DMA((2,)),
        ],
        compiler_params=pltpu.CompilerParams(
            collective_id=1, has_side_effects=True, vmem_limit_bytes=48 * 1024 * 1024
        ),
    )(part, prob)


def per_device(
    output_grad,
    layer_input,
    expert_ids,
    route_probs,
    gate_weight,
    up_weight,
    down_weight,
    saved_inputs,
    saved_gate_grad,
    saved_up_grad,
    saved_counts,
):
    ep_count = lax.axis_size("ep")
    sections = lax.axis_size("section")
    me = lax.axis_index("ep")
    w_gate = gate_weight[0]
    w_up = up_weight[0]
    w_down = down_weight[0]
    local_experts = w_gate.shape[0]
    experts_all = local_experts * ep_count
    slots_all = saved_inputs.shape[2]
    capacity = slots_all // ep_count
    tok_rows = expert_ids.shape[1]
    top_count = expert_ids.shape[2]
    width = output_grad.shape[2]

    small = jnp.concatenate([expert_ids[0].astype(BF16), route_probs[0]], axis=1).T
    grad_all, input_all, small_all = gather_tokens(
        ep_count, output_grad[0], layer_input[0], small
    )

    live = jnp.arange(capacity, dtype=jnp.int32)[None, None, :] < saved_counts[0][:, :, None]
    masked = saved_inputs[0] * live.reshape(local_experts, slots_all).astype(BF16)[:, :, None]
    gate_part = jnp.einsum(
        "esd,esf->edf", masked, saved_gate_grad[0], preferred_element_type=F32
    ).astype(BF16)
    up_part = jnp.einsum(
        "esd,esf->edf", masked, saved_up_grad[0], preferred_element_type=F32
    ).astype(BF16)

    ids_all = small_all[:, :top_count].astype(jnp.int32)
    probs_all = small_all[:, top_count:].astype(F32)
    mine = me * local_experts + jnp.arange(local_experts, dtype=jnp.int32)
    hit = ids_all[:, None, :, :] == mine[None, :, None, None]
    member = jnp.any(hit, axis=2)
    prob = jnp.sum(jnp.where(hit, probs_all[:, None], 0.0), axis=2)
    lower = jnp.tril(jnp.ones((tok_rows, tok_rows), BF16), -1)
    before = jnp.einsum("sen,tn->set", member.astype(BF16), lower, preferred_element_type=F32)
    slot = jnp.where(member, before.astype(jnp.int32), -1)
    chosen = slot[:, :, None, :] == jnp.arange(capacity, dtype=jnp.int32)[None, None, :, None]
    pick = chosen.astype(BF16).reshape(ep_count, local_experts * capacity, tok_rows)
    put = jnp.where(chosen, prob[:, :, None, :], 0.0).astype(BF16)
    put = put.reshape(ep_count, local_experts * capacity, tok_rows)

    def spread(tokens):
        sent = jnp.einsum("spt,std->spd", pick, tokens, preferred_element_type=F32).astype(BF16)
        sent = sent.reshape(ep_count, local_experts, capacity, width)
        return sent.transpose(1, 0, 2, 3).reshape(local_experts, slots_all, width)

    grad_part = spread(grad_all)
    input_part = spread(input_all)

    gate_pre = jnp.einsum("epd,edf->epf", input_part, w_gate, preferred_element_type=F32)
    up_pre = jnp.einsum("epd,edf->epf", input_part, w_up, preferred_element_type=F32)
    sigma = jax.nn.sigmoid(gate_pre)
    active = gate_pre * sigma
    hidden = active * up_pre
    hidden_grad = jnp.einsum("epd,efd->epf", grad_part, w_down, preferred_element_type=F32)
    slot_prob = jnp.sum(hidden_grad * hidden, axis=2).astype(BF16)
    gate_grad = (hidden_grad * up_pre * sigma * (1.0 + gate_pre * (1.0 - sigma))).astype(BF16)
    up_grad = (hidden_grad * active).astype(BF16)
    slot_grad = jnp.einsum("epf,edf->epd", gate_grad, w_gate, preferred_element_type=F32)
    slot_grad = slot_grad + jnp.einsum("epf,edf->epd", up_grad, w_up, preferred_element_type=F32)
    slot_grad = slot_grad.astype(BF16).reshape(local_experts, ep_count, capacity, width)
    slot_grad = slot_grad.transpose(1, 0, 2, 3).reshape(ep_count, -1, width)
    token_grad = jnp.einsum("spt,spd->std", put, slot_grad, preferred_element_type=F32)
    slot_prob = slot_prob.reshape(local_experts, ep_count, capacity)
    by_slot = chosen.astype(BF16)
    token_prob = jnp.einsum("sect,esc->set", by_slot, slot_prob, preferred_element_type=F32)
    upstream, prob_back = scatter_tokens(
        ep_count, sections, token_grad.astype(BF16), token_prob.astype(BF16)
    )
    prob_back = prob_back.reshape(experts_all, tok_rows)
    own = expert_ids[0][None, :, :] == jnp.arange(experts_all, dtype=jnp.int32)[:, None, None]
    prob_part = jnp.sum(jnp.where(own, prob_back[:, :, None].astype(F32), 0.0), axis=0)
    prob_part = prob_part.astype(BF16)
    upstream = upstream[None]
    return (upstream, prob_part[None], gate_part[None], up_part[None])


def solution(mesh):
    three = P("section", "ep", None)
    four = P("section", "ep", None, None)
    return jax.shard_map(
        per_device,
        mesh=mesh,
        in_specs=(three, three, three, three, four, four, four, four, four, four, three),
        out_specs=(three, three, four, four),
        check_vma=False,
    )
```

```python
import functools

import jax
import jax.numpy as jnp
from jax import lax
from jax.experimental import pallas as pl
from jax.experimental.pallas import tpu as pltpu
from jax.sharding import PartitionSpec as P

F32 = jnp.float32
BF16 = jnp.bfloat16
MESH = pl.DeviceIdType.MESH
VMEM = pl.BlockSpec(memory_space=pltpu.VMEM)
ANY = pl.BlockSpec(memory_space=pl.ANY)


class Copies:
    def __init__(self, send, recv):
        self.send, self.recv, self.used, self.items = send, recv, 0, []

    def start(self, src, dst, target, when=None):
        at = self.used
        self.used += 1
        copy = pltpu.make_async_remote_copy(
            src_ref=src,
            dst_ref=dst,
            send_sem=self.send.at[at],
            recv_sem=self.recv.at[at],
            device_id={"ep": target},
            device_id_type=MESH,
        )
        self.items.append((copy, when))
        guarded(when, copy.start)
        return copy

    def finish(self):
        for copy, when in self.items:
            guarded(when, copy.wait_send)


def guarded(when, act):
    if when is None:
        act()
    else:
        pl.when(when)(act)


def place_of(count):
    me = lax.axis_index("ep")
    outer, inner = me // 2, me % 2
    line = count // 2
    up = ((outer + 1) % line) * 2 + inner
    down = ((outer + line - 1) % line) * 2 + inner
    return me, outer, inner, line, (up, down), outer * 2 + 1 - inner


def gather_copies(count):
    line = count // 2
    return 12 * (line - 1) + 3 + (count - 1)


def weight_tile(live, held, saved, outs, expert):
    mask = live[expert][:, :1]
    grads = [ref[expert] * mask for ref in saved]
    tile = 256

    def body(at, carry):
        columns = pl.ds(pl.multiple_of(at * tile, tile), tile)
        rows = held[expert, :, columns]
        for grad, out in zip(grads, outs):
            out[expert, columns, :] = lax.dot_general(
                rows, grad, (((0,), (0,)), ((), ())), preferred_element_type=F32
            ).astype(BF16)
        return carry

    lax.fori_loop(0, held.shape[2] // tile, body, 0)


def gather_kernel(
    count, g, x, s, live, held_in, gate_in, up_in, g_all, x_all, s_all, gate_out, up_out, held,
    gate_held, up_held, local, send, recv,
):
    me, outer, inner, line, sides, partner = place_of(count)
    width = g.shape[1]
    cut = max(width * 3 // 1024, 1) * 128
    copies = Copies(send, recv)
    own = [
        pltpu.make_async_copy(g, g_all.at[me], local.at[0]),
        pltpu.make_async_copy(x, x_all.at[me], local.at[1]),
        pltpu.make_async_copy(s, s_all.at[me], local.at[2]),
    ]
    loads = [
        pltpu.make_async_copy(src, dst, local.at[3 + at])
        for at, (src, dst) in enumerate(((held_in, held), (gate_in, gate_held), (up_in, up_held)))
    ]
    for copy in own + loads:
        copy.start()
    barrier = pltpu.get_barrier_semaphore()
    for away in range(1, count):
        pl.semaphore_signal(
            barrier, inc=1, device_id={"ep": (me + away) % count}, device_id_type=MESH
        )
    pl.semaphore_wait(barrier, count - 1)
    everything, few, many = pl.ds(0, width), pl.ds(0, cut), pl.ds(cut, width - cut)

    def block(step, side):
        return (outer + (-step if side == 0 else step) + 2 * line) % line

    def arrives(step, side):
        return outer >= step + 1 if side == 0 else outer + step + 1 <= line - 1

    def leaves(step, side):
        if side == 0:
            return jnp.logical_and(outer >= step, outer < line - 1)
        return jnp.logical_and(outer + step <= line - 1, outer > 0)

    def hop(ref, all_ref, columns, step, side, row):
        dst = all_ref.at[block(step, side) * 2 + row, :, columns]
        source = dst if ref is None else ref.at[:, columns]
        return copies.start(source, dst, sides[side], leaves(step, side))

    def take(copy, step, side):
        guarded(arrives(step, side), copy.wait_recv)

    side_list = (0, 1)
    other = 1 - inner
    pieces = ((x, x_all, everything), (g, g_all, many))
    now = {}
    g_across = copies.start(g.at[:, few], g_all.at[me, :, few], partner)
    for at, (ref, all_ref, columns) in enumerate(pieces):
        for side in side_list:
            now[at, side] = hop(ref, all_ref, columns, 0, side, inner)
    for side in side_list:
        now[2, side] = hop(g, g_all, few, 0, side, inner)
    late = [
        (copies.start(x, x_all.at[me], partner), None),
        (copies.start(g.at[:, many], g_all.at[me, :, many], partner), None),
    ]
    for away in range(1, count):
        late.append((copies.start(s, s_all.at[me], (me + away) % count), None))
    experts = list(range(held.shape[0]))
    for copy in loads:
        copy.wait()

    def work():
        if experts:
            weight_tile(live, held, (gate_held, up_held), (gate_out, up_out), experts.pop(0))

    work()
    g_across.wait_recv()
    for side in side_list:
        now[3, side] = hop(None, g_all, few, 0, side, other)
    for step in range(line - 1):
        more = step < line - 2
        for at in range(4):
            row = other if at == 3 else inner
            all_ref, columns = pieces[at][1:] if at < 2 else (g_all, few)
            for side in side_list:
                take(now[at, side], step, side)
                if more:
                    now[at, side] = hop(None, all_ref, columns, step + 1, side, row)
                if at < 2:
                    got = all_ref.at[block(step + 1, side) * 2 + inner, :, columns]
                    has = arrives(step, side)
                    late.append((copies.start(got, got, partner, has), has))
            if at % 2 == 1:
                work()
    while experts:
        work()
    for copy, when in late:
        guarded(when, copy.wait_recv)
    copies.finish()
    for copy in own:
        copy.wait()


def gather_tokens(count, g, x, s, live, held, gate, up):
    pairs = gather_copies(count)
    grads = jax.ShapeDtypeStruct((held.shape[0], held.shape[2], gate.shape[2]), BF16)
    return pl.pallas_call(
        functools.partial(gather_kernel, count),
        out_shape=[jax.ShapeDtypeStruct((count,) + a.shape, a.dtype) for a in (g, x, s)]
        + [grads, grads],
        in_specs=[VMEM] * 4 + [ANY] * 3,
        out_specs=[ANY] * 3 + [VMEM] * 2,
        scratch_shapes=[
            pltpu.VMEM(held.shape, BF16),
            pltpu.VMEM(gate.shape, BF16),
            pltpu.VMEM(up.shape, BF16),
            pltpu.SemaphoreType.DMA((6,)),
            pltpu.SemaphoreType.DMA((pairs,)),
            pltpu.SemaphoreType.DMA((pairs,)),
        ],
        compiler_params=pltpu.CompilerParams(
            collective_id=0, has_side_effects=True, vmem_limit_bytes=48 * 1024 * 1024
        ),
    )(g, x, s, live, held, gate, up)


def scatter_copies(count):
    line = count // 2
    return line + 1 + (count - 1)


def add(a, b):
    return (a.astype(F32) + b.astype(F32)).astype(BF16)


def scatter_kernel(
    count, sections, part, prob, out, prob_out, a_sum, a_side, a_take, b_sum, b_side, land_a,
    land_b, send, recv, line_send, line_recv, shift_send, shift_recv,
):
    me, outer, inner, line, sides, partner = place_of(count)
    section = lax.axis_index("section")
    cut = a_sum.shape[3]
    copies = Copies(send, recv)
    barrier = pltpu.get_barrier_semaphore()
    for away in range(1, count):
        pl.semaphore_signal(
            barrier, inc=1, device_id={"ep": (me + away) % count}, device_id_type=MESH
        )
    for away in (1, sections - 1):
        pl.semaphore_signal(
            barrier, inc=1, device_id={"section": (section + away) % sections}, device_id_type=MESH
        )
    pl.semaphore_wait(barrier, count + 1)
    other = 1 - inner
    low, high = pl.ds(0, cut), pl.ds(cut, part.shape[2] - cut)

    def goal(at):
        mixed = line - 1 - at // 2 if at % 2 == 0 else at // 2
        return jnp.where(outer == 0, line - 1 - at, jnp.where(outer == line - 1, at, mixed))

    across = [
        copies.start(part.at[goal(at) * 2 + other, :, high], b_sum.at[goal(at)], partner)
        for at in range(line)
    ]
    tiny = [
        copies.start(prob.at[(me + away) % count], prob_out.at[me], (me + away) % count)
        for away in range(1, count)
    ]
    prob_out[me] = prob[me]

    def line_copy(kind, source, side_ref, side, place):
        return pltpu.make_async_remote_copy(
            src_ref=source.at[place],
            dst_ref=side_ref.at[side, place],
            send_sem=line_send.at[kind, side, place],
            recv_sem=line_recv.at[kind, side, place],
            device_id={"ep": sides[side]},
            device_id_type=MESH,
        )

    def collect(kind, total, side_ref, side, place):
        line_copy(kind, total, side_ref, side, place).wait_recv()
        total[place] = add(total[place], side_ref[side, place])

    def advance(kind, total, side_ref, place):
        @pl.when(jnp.logical_and(place >= outer, outer > 0))
        def _():
            collect(kind, total, side_ref, 0, place)

        @pl.when(jnp.logical_and(place <= outer, outer < line - 1))
        def _():
            collect(kind, total, side_ref, 1, place)

        @pl.when(place > outer)
        def _():
            line_copy(kind, total, side_ref, 0, place).start()

        @pl.when(place < outer)
        def _():
            line_copy(kind, total, side_ref, 1, place).start()

    for at in range(line):
        place = goal(at)
        for kind, row in ((0, other), (1, inner)):
            a_sum[kind, place] = part[place * 2 + row, :, :cut]
            advance(kind, a_sum.at[kind], a_side.at[kind], place)
    a_across = copies.start(a_sum.at[0, outer], a_take, partner)
    for at in range(line):
        place = goal(at)
        across[at].wait_recv()
        b_sum[place] = add(b_sum[place], part[place * 2 + inner, :, cut:])
        advance(2, b_sum, b_side, place)

    def shift(column, source, land):
        return pltpu.make_async_remote_copy(
            src_ref=source,
            dst_ref=land,
            send_sem=shift_send.at[column],
            recv_sem=shift_recv.at[column],
            device_id={"section": (section + sections - 1) % sections},
            device_id_type=MESH,
        )

    a_across.wait_recv()
    a_sum[1, outer] = add(a_sum[1, outer], a_take[...])
    shifts = (shift(0, a_sum.at[1, outer], land_a), shift(1, b_sum.at[outer], land_b))

    @pl.when(section > 0)
    def _():
        for copy in shifts:
            copy.start()

    for copy in tiny:
        copy.wait_recv()
    copies.finish()
    for place in range(line):
        for kind, total, side_ref in (
            (0, a_sum.at[0], a_side.at[0]),
            (1, a_sum.at[1], a_side.at[1]),
            (2, b_sum, b_side),
        ):
            guarded(place > outer, line_copy(kind, total, side_ref, 0, place).wait_send)
            guarded(place < outer, line_copy(kind, total, side_ref, 1, place).wait_send)

    @pl.when(section > 0)
    def _():
        for copy in shifts:
            copy.wait_send()

    @pl.when(section < sections - 1)
    def _():
        shifts[0].wait_recv()
        out[:, :cut] = land_a[...]
        shifts[1].wait_recv()
        out[:, cut:] = land_b[...]

    @pl.when(section == sections - 1)
    def _():
        out[...] = jnp.zeros_like(out)


def scatter_tokens(count, sections, part, prob):
    pairs = scatter_copies(count)
    line = count // 2
    _, tokens, width = part.shape
    cut = max(width // 1024, 1) * 128
    rest = width - cut
    return pl.pallas_call(
        functools.partial(scatter_kernel, count, sections),
        out_shape=[
            jax.ShapeDtypeStruct((tokens, width), BF16),
            jax.ShapeDtypeStruct(prob.shape, prob.dtype),
        ],
        in_specs=[VMEM] * 2,
        out_specs=[VMEM] * 2,
        scratch_shapes=[
            pltpu.VMEM((2, line, tokens, cut), BF16),
            pltpu.VMEM((2, 2, line, tokens, cut), BF16),
            pltpu.VMEM((tokens, cut), BF16),
            pltpu.VMEM((line, tokens, rest), BF16),
            pltpu.VMEM((2, line, tokens, rest), BF16),
            pltpu.VMEM((tokens, cut), BF16),
            pltpu.VMEM((tokens, rest), BF16),
            pltpu.SemaphoreType.DMA((pairs,)),
            pltpu.SemaphoreType.DMA((pairs,)),
            pltpu.SemaphoreType.DMA((3, 2, line)),
            pltpu.SemaphoreType.DMA((3, 2, line)),
            pltpu.SemaphoreType.DMA((2,)),
            pltpu.SemaphoreType.DMA((2,)),
        ],
        compiler_params=pltpu.CompilerParams(
            collective_id=1, has_side_effects=True, vmem_limit_bytes=48 * 1024 * 1024
        ),
    )(part, prob)


def per_device(
    output_grad,
    layer_input,
    expert_ids,
    route_probs,
    gate_weight,
    up_weight,
    down_weight,
    saved_inputs,
    saved_gate_grad,
    saved_up_grad,
    saved_counts,
):
    ep_count = lax.axis_size("ep")
    sections = lax.axis_size("section")
    me = lax.axis_index("ep")
    w_gate = gate_weight[0]
    w_up = up_weight[0]
    w_down = down_weight[0]
    local_experts = w_gate.shape[0]
    experts_all = local_experts * ep_count
    slots_all = saved_inputs.shape[2]
    capacity = slots_all // ep_count
    tok_rows = expert_ids.shape[1]
    top_count = expert_ids.shape[2]
    width = output_grad.shape[2]

    small = jnp.concatenate([expert_ids[0].astype(BF16), route_probs[0]], axis=1).T
    live = jnp.arange(capacity, dtype=jnp.int32)[None, None, :] < saved_counts[0][:, :, None]
    live = jnp.broadcast_to(
        live.reshape(local_experts, slots_all, 1).astype(BF16), (local_experts, slots_all, 128)
    )
    grad_all, input_all, small_all, gate_part, up_part = gather_tokens(
        ep_count,
        output_grad[0],
        layer_input[0],
        small,
        live,
        saved_inputs[0],
        saved_gate_grad[0],
        saved_up_grad[0],
    )

    ids_all = small_all[:, :top_count].astype(jnp.int32)
    probs_all = small_all[:, top_count:].astype(F32)
    mine = me * local_experts + jnp.arange(local_experts, dtype=jnp.int32)
    hit = ids_all[:, None, :, :] == mine[None, :, None, None]
    member = jnp.any(hit, axis=2)
    prob = jnp.sum(jnp.where(hit, probs_all[:, None], 0.0), axis=2)
    lower = jnp.tril(jnp.ones((tok_rows, tok_rows), BF16), -1)
    before = jnp.einsum("sen,tn->set", member.astype(BF16), lower, preferred_element_type=F32)
    slot = jnp.where(member, before.astype(jnp.int32), -1)
    chosen = slot[:, :, None, :] == jnp.arange(capacity, dtype=jnp.int32)[None, None, :, None]
    pick = chosen.astype(BF16).reshape(ep_count, local_experts * capacity, tok_rows)
    put = jnp.where(chosen, prob[:, :, None, :], 0.0).astype(BF16)
    put = put.reshape(ep_count, local_experts * capacity, tok_rows)

    def spread(tokens):
        sent = jnp.einsum("spt,std->spd", pick, tokens, preferred_element_type=F32).astype(BF16)
        sent = sent.reshape(ep_count, local_experts, capacity, width)
        return sent.transpose(1, 0, 2, 3).reshape(local_experts, slots_all, width)

    grad_part = spread(grad_all)
    input_part = spread(input_all)

    gate_pre = jnp.einsum("epd,edf->epf", input_part, w_gate, preferred_element_type=F32)
    up_pre = jnp.einsum("epd,edf->epf", input_part, w_up, preferred_element_type=F32)
    sigma = jax.nn.sigmoid(gate_pre)
    active = gate_pre * sigma
    hidden = active * up_pre
    hidden_grad = jnp.einsum("epd,efd->epf", grad_part, w_down, preferred_element_type=F32)
    slot_prob = jnp.sum(hidden_grad * hidden, axis=2).astype(BF16)
    gate_grad = (hidden_grad * up_pre * sigma * (1.0 + gate_pre * (1.0 - sigma))).astype(BF16)
    up_grad = (hidden_grad * active).astype(BF16)
    slot_grad = jnp.einsum("epf,edf->epd", gate_grad, w_gate, preferred_element_type=F32)
    slot_grad = slot_grad + jnp.einsum("epf,edf->epd", up_grad, w_up, preferred_element_type=F32)
    slot_grad = slot_grad.astype(BF16).reshape(local_experts, ep_count, capacity, width)
    slot_grad = slot_grad.transpose(1, 0, 2, 3).reshape(ep_count, -1, width)
    token_grad = jnp.einsum("spt,spd->std", put, slot_grad, preferred_element_type=F32)
    slot_prob = slot_prob.reshape(local_experts, ep_count, capacity)
    by_slot = chosen.astype(BF16)
    token_prob = jnp.einsum("sect,esc->set", by_slot, slot_prob, preferred_element_type=F32)
    upstream, prob_back = scatter_tokens(
        ep_count, sections, token_grad.astype(BF16), token_prob.astype(BF16)
    )
    prob_back = prob_back.reshape(experts_all, tok_rows)
    own = expert_ids[0][None, :, :] == jnp.arange(experts_all, dtype=jnp.int32)[:, None, None]
    prob_part = jnp.sum(jnp.where(own, prob_back[:, :, None].astype(F32), 0.0), axis=0)
    prob_part = prob_part.astype(BF16)
    upstream = upstream[None]
    return (upstream, prob_part[None], gate_part[None], up_part[None])


def solution(mesh):
    three = P("section", "ep", None)
    four = P("section", "ep", None, None)
    return jax.shard_map(
        per_device,
        mesh=mesh,
        in_specs=(three, three, three, three, four, four, four, four, four, four, three),
        out_specs=(three, three, four, four),
        check_vma=False,
    )
```
